16 devices in a mesh: rep: 4 (over y, z, core), dp: 4 (over x).
Axes of the slice: x: 4, y: 2, z: 1, core: 2. Of those that a mesh axis runs over, the one named last changes fastest.
The devices are a block of a 4x4x8 slice.
Arguments:
- x: bfloat16 [16, 4096, 640], P(('rep', 'dp')), parts along dimension 0
- dy: bfloat16 [16, 4096, 640], P(('rep', 'dp')), parts along dimension 0
- w_gate: bfloat16 [2, 640, 2048], replicated
- w_up: bfloat16 [2, 640, 2048], replicated
- w_down: bfloat16 [2, 2048, 640], replicated
- m_w_gate: float32 [2, 640, 2048], P(None, 'dp')
- m_w_up: float32 [2, 640, 2048], P(None, 'dp')
- m_w_down: float32 [2, 2048, 640], P(None, 'dp')
- v_w_gate: float32 [2, 640, 2048], P(None, 'dp')
- v_w_up: float32 [2, 640, 2048], P(None, 'dp')
- v_w_down: float32 [2, 2048, 640], P(None, 'dp')
Outputs:
- output 1: bfloat16 [8, 640, 2048], P('rep'), parts along dimension 0
- output 2: bfloat16 [8, 640, 2048], P('rep'), parts along dimension 0
- output 3: bfloat16 [8, 2048, 640], P('rep'), parts along dimension 0
- output 4: float32 [8, 640, 2048], P('rep', 'dp'), parts along dimension 0
- output 5: float32 [8, 640, 2048], P('rep', 'dp'), parts along dimension 0
- output 6: float32 [8, 2048, 640], P('rep', 'dp'), parts along dimension 0
- output 7: float32 [8, 640, 2048], P('rep', 'dp'), parts along dimension 0
- output 8: float32 [8, 640, 2048], P('rep', 'dp'), parts along dimension 0
- output 9: float32 [8, 2048, 640], P('rep', 'dp'), parts along dimension 0
There are 4 independent parts. The reference program is written for one: setup_inputs(seed, part) draws one part's arguments, and reference() takes and returns one part's arrays. A program takes and returns all parts, laid end to end along the dimension named above; an argument that names none is the same for every part.
All inputs are finite; a program needn't handle non-finite values.
Results may differ from the reference program's by a relative error of at most 0.022.
Values are sent between devices in bfloat16 or wider.
A program may use at most 768 MiB of HBM per device.

```python
import jax
import jax.numpy as jnp
from jax import lax

SEQUENCES = 4
TOKENS = 4096
D = 640
FF = 2048
LAYERS = 2
NAMES = ("w_gate", "w_up", "w_down")
SHAPES = {"w_gate": (LAYERS, D, FF), "w_up": (LAYERS, D, FF), "w_down": (LAYERS, FF, D)}


def bump(key, n, height):
    away = (jnp.arange(n, dtype=jnp.int32) - jax.random.randint(key, (), 0, n, jnp.int32)) % n
    return jnp.where(away < n // 8, height, 1.0)


def together(key, own, strength):
    shared = jax.random.normal(key, own.shape[1:], jnp.float32)
    return (own + strength * shared) * lax.rsqrt(1 + strength * strength)


def setup_inputs(seed: int = 0, part: int = 0) -> dict:
    kx, kdy, ka, kb, kz, kf, kh, kl, *keys = jax.random.split(jax.random.key(seed), 8 + 3 * len(NAMES))
    kx, kdy, ka, kb = (jax.random.fold_in(k, part) for k in (kx, kdy, ka, kb))
    kw, km, kv = (keys[i::3] for i in range(3))
    shape = (SEQUENCES, TOKENS, D)
    much_x, much_dy = jax.random.uniform(kz, (2,), jnp.float32, 0.0, 1.0)
    loud = 2.0 ** jax.random.uniform(jax.random.fold_in(kz, 1), (), jnp.float32, -1.0, 2.0)
    layers = 2.0 ** jax.random.uniform(kl, (LAYERS, 1, 1), jnp.float32, -1.0, 1.0)
    x = together(ka, jax.random.normal(kx, shape, jnp.float32), much_x) * bump(kf, D, 4.0)
    dy = together(kb, jax.random.normal(kdy, shape, jnp.float32), much_dy)
    drawn = {"x": x.astype(jnp.bfloat16), "dy": (loud * dy * (SEQUENCES * TOKENS) ** -0.5).astype(jnp.bfloat16)}
    for key, name in zip(kw, NAMES, strict=True):
        w = jax.random.normal(key, SHAPES[name], jnp.float32) * SHAPES[name][1] ** -0.5
        drawn[name] = (w * {"w_gate": 1.0, "w_up": bump(kh, FF, 4.0), "w_down": layers}[name]).astype(jnp.bfloat16)
    for key, name in zip(km, NAMES, strict=True):
        drawn[f"m_{name}"] = 0.1 * jax.random.normal(key, SHAPES[name], jnp.float32)
    for key, name in zip(kv, NAMES, strict=True):
        drawn[f"v_{name}"] = jax.random.uniform(key, SHAPES[name], jnp.float32, 0.005, 0.015)
    return drawn


def matmul(a, w):
    return jnp.dot(a, w, preferred_element_type=jnp.float32).astype(jnp.bfloat16)


def normed(h):
    wide = h.astype(jnp.float32)
    scale = lax.rsqrt(jnp.mean(wide**2, -1, keepdims=True) + 1e-6)
    return (wide * scale).astype(jnp.bfloat16)


def layer(h, w):
    a = normed(h)
    gate = jnp.dot(a, w["w_gate"], preferred_element_type=jnp.float32)
    up = jnp.dot(a, w["w_up"], preferred_element_type=jnp.float32)
    return h + matmul((jax.nn.silu(gate) * up).astype(jnp.bfloat16), w["w_down"])


def adamw(w, m, v, g):
    m = 0.9 * m + 0.1 * g
    v = 0.95 * v + 0.05 * g * g
    step = m * lax.rsqrt(v + 1e-8) + 0.1 * w
    return (w - 0.02 * step).astype(jnp.bfloat16), m, v


def stack(weights, h):
    return lax.scan(lambda h, w: (layer(h, w), None), h, weights)[0]


def reference(x, dy, w_gate, w_up, w_down, m_w_gate, m_w_up, m_w_down, v_w_gate, v_w_up, v_w_down):
    weights = dict(zip(NAMES, (w_gate, w_up, w_down), strict=True))

    def take(so_far, sequence):
        h, by_y = sequence
        _, back = jax.vjp(lambda w: stack(w, h), weights)
        return jax.tree.map(lambda total, term: total + term.astype(jnp.float32), so_far, back(by_y)[0]), None

    none_yet = {name: jnp.zeros(w.shape, jnp.float32) for name, w in weights.items()}
    by_weights, _ = lax.scan(take, none_yet, (x, dy))
    gradients = [by_weights[name].astype(jnp.bfloat16).astype(jnp.float32) for name in NAMES]
    new = [
        adamw(w.astype(jnp.float32), m, v, g)
        for w, m, v, g in zip((w_gate, w_up, w_down), (m_w_gate, m_w_up, m_w_down), (v_w_gate, v_w_up, v_w_down), gradients, strict=True)
    ]
    return tuple(one[which] for which in range(3) for one in new)
```

```python
import functools

import jax
import jax.numpy as jnp
from jax import lax
from jax.experimental import pallas as pl
from jax.experimental.pallas import tpu as pltpu
from jax.sharding import PartitionSpec as P

F32, BF16 = jnp.float32, jnp.bfloat16
TILE = 512
LANES = 128


def nn(a, b):
    return lax.dot_general(a, b, (((1,), (0,)), ((), ())), preferred_element_type=F32)


def nt(a, b):
    return lax.dot_general(a, b, (((1,), (1,)), ((), ())), preferred_element_type=F32)


def tn(a, b):
    return lax.dot_general(a, b, (((0,), (0,)), ((), ())), preferred_element_type=F32)


def normed(h):
    wide = h.astype(F32)
    scale = lax.rsqrt(jnp.mean(wide * wide, -1, keepdims=True) + 1e-6)
    return (wide * scale).astype(BF16)


def normed_back(h, by_a):
    wide = h.astype(F32)
    scale = lax.rsqrt(jnp.mean(wide * wide, -1, keepdims=True) + 1e-6)
    along = jnp.mean(by_a * wide, -1, keepdims=True)
    return (scale * by_a - wide * (scale * scale * scale * along)).astype(BF16)


def kernel(
    n,
    x_in, dy_in, wg_in, wu_in, wd_in, mg_in, mu_in, md_in, vg_in, vu_in, vd_in,
    wg_out, wu_out, wd_out, mg_out, mu_out, md_out, vg_out, vu_out, vd_out,
    x, h1, dy, a, acc, accgu, accd, wg, wu, wd,
    s1gu, s1d, r1gu, r1d, s2gu, s2d, r2gu, r2d, wngu, wnd, mvgu, mvd,
    tile_sem, w_sem, ld_sem, st_sem,
    rs1_send, rs1_recv, rs2_send, rs2_recv, ag1_send, ag1_recv, ag2_send, ag2_recv,
):
    tokens, d_model = x.shape
    ff = wg_in.shape[2]
    tiles = tokens // TILE
    share = ff // n
    chunks = share // LANES
    chunk = n * LANES
    rows = d_model // n
    half = LANES // 2

    me = lax.axis_index("dp")
    right, left, far = (lax.rem(me + k, n) for k in (1, n - 1, n // 2))

    def cols_of(owner, i):
        return pl.ds(pl.multiple_of(owner * share + i * LANES, LANES), LANES)

    def rows_of(owner):
        return pl.ds(pl.multiple_of(owner * rows, rows), rows)

    def units_of(owner):
        return pl.ds(pl.multiple_of(owner * LANES, LANES), LANES)

    def same(ref, sem):
        return pltpu.make_async_copy(ref, ref, sem)

    def part(owner):
        return slice(owner * LANES, (owner + 1) * LANES)

    def load_w(k):
        slot, layer, i = k % 2, (k // chunks) % 2, k % chunks
        for o in range(n):
            pltpu.make_async_copy(wg_in.at[layer, :, cols_of(o, i)], wg.at[slot, :, part(o)], w_sem.at[slot, 0]).start()
            pltpu.make_async_copy(wu_in.at[layer, :, cols_of(o, i)], wu.at[slot, :, part(o)], w_sem.at[slot, 1]).start()
            pltpu.make_async_copy(wd_in.at[layer, cols_of(o, i), :], wd.at[slot, part(o), :], w_sem.at[slot, 2]).start()

    def wait_w(k):
        slot = k % 2
        for j, ref in enumerate((wg, wu, wd)):
            same(ref.at[slot], w_sem.at[slot, j]).wait()

    def where(c):
        return c % 2, 1 - c // chunks, c % chunks

    def load_mvw(c):
        s, layer, i = where(c)
        for j, (m_in, v_in, w_in) in enumerate(((mg_in, vg_in, wg_in), (mu_in, vu_in, wu_in))):
            for o in range(n):
                pltpu.make_async_copy(m_in.at[layer, :, cols_of(o, i)], mvgu.at[s, 0, j, :, part(o)], ld_sem.at[s, 0]).start()
                pltpu.make_async_copy(v_in.at[layer, :, cols_of(o, i)], mvgu.at[s, 1, j, :, part(o)], ld_sem.at[s, 0]).start()
                pltpu.make_async_copy(w_in.at[layer, rows_of(me), cols_of(o, i)], wngu.at[s, j, :, part(o)], ld_sem.at[s, 2]).start()
        mine = pl.ds(pl.multiple_of(i * LANES, LANES), LANES)
        pltpu.make_async_copy(md_in.at[layer, mine, :], mvd.at[s, 0], ld_sem.at[s, 1]).start()
        pltpu.make_async_copy(vd_in.at[layer, mine, :], mvd.at[s, 1], ld_sem.at[s, 1]).start()
        pltpu.make_async_copy(wd_in.at[layer, cols_of(me, i), :], wnd.at[s], ld_sem.at[s, 3]).start()

    def wait_four(c, sem):
        s = c % 2
        for j, ref in enumerate((mvgu, mvd, wngu, wnd)):
            same(ref.at[s], sem.at[s, j]).wait()

    def store_mvw(c):
        s, layer, i = where(c)
        for j, (m_out, v_out, w_out) in enumerate(((mg_out, vg_out, wg_out), (mu_out, vu_out, wu_out))):
            for o in range(n):
                pltpu.make_async_copy(mvgu.at[s, 0, j, :, part(o)], m_out.at[layer, :, cols_of(o, i)], st_sem.at[s, 0]).start()
                pltpu.make_async_copy(mvgu.at[s, 1, j, :, part(o)], v_out.at[layer, :, cols_of(o, i)], st_sem.at[s, 0]).start()
                pltpu.make_async_copy(wngu.at[s, j, :, part(o)], w_out.at[layer, rows_of(me), cols_of(o, i)], st_sem.at[s, 2]).start()
        mine = pl.ds(pl.multiple_of(i * LANES, LANES), LANES)
        pltpu.make_async_copy(mvd.at[s, 0], md_out.at[layer, mine, :], st_sem.at[s, 1]).start()
        pltpu.make_async_copy(mvd.at[s, 1], vd_out.at[layer, mine, :], st_sem.at[s, 1]).start()
        pltpu.make_async_copy(wnd.at[s], wd_out.at[layer, cols_of(me, i), :], st_sem.at[s, 3]).start()

    def send(src, dst, send_sem, recv_sem, to):
        pltpu.make_async_remote_copy(
            src_ref=src, dst_ref=dst, send_sem=send_sem, recv_sem=recv_sem,
            device_id={"dp": to}, device_id_type=pl.DeviceIdType.MESH,
        ).start()

    def sum_1(c):
        s = c % 2
        for j, to in enumerate((right, left)):
            s1gu[j] = accgu[s, j, rows_of(far), :].astype(BF16)
        down = accd[s, :, units_of(far)].T
        s1d[0] = down[:half].astype(BF16)
        s1d[1] = down[half:].astype(BF16)
        for j, to in enumerate((right, left)):
            send(s1gu.at[j], r1gu.at[s, j], rs1_send.at[j, 0], rs1_recv.at[s, j, 0], to)
            send(s1d.at[j], r1d.at[s, j], rs1_send.at[j, 1], rs1_recv.at[s, j, 1], to)

    def sum_2(c):
        s = c % 2
        for j, to in enumerate((right, left)):
            same(s1gu.at[j], rs1_send.at[j, 0]).wait()
            same(s1d.at[j], rs1_send.at[j, 1]).wait()
            same(r1gu.at[s, j], rs1_recv.at[s, j, 0]).wait()
            same(r1d.at[s, j], rs1_recv.at[s, j, 1]).wait()
            for k in range(2):
                total = accgu[s, k, rows_of(to), :]
                if k == j:
                    total += r1gu[s, j].astype(F32)
                s2gu[j, k] = total.astype(BF16)
            down = accd[s, :, units_of(to)].T
            for k in range(2):
                total = down[k * half : (k + 1) * half]
                if k == j:
                    total += r1d[s, j].astype(F32)
                s2d[j, k * half : (k + 1) * half] = total.astype(BF16)
            send(s2gu.at[j], r2gu.at[s, j], rs2_send.at[j, 0], rs2_recv.at[s, j, 0], to)
            send(s2d.at[j], r2d.at[s, j], rs2_send.at[j, 1], rs2_recv.at[s, j, 1], to)

    def adamw(w, m, v, g):
        g = g.astype(BF16).astype(F32)
        m = 0.9 * m + 0.1 * g
        v = 0.95 * v + 0.05 * g * g
        w = w.astype(F32)
        return (w - 0.02 * (m * lax.rsqrt(v + 1e-8) + 0.1 * w)).astype(BF16), m, v

    def sum_3(c):
        s, layer, i = where(c)
        for j in range(2):
            same(s2gu.at[j], rs2_send.at[j, 0]).wait()
            same(s2d.at[j], rs2_send.at[j, 1]).wait()
            same(r2gu.at[s, j], rs2_recv.at[s, j, 0]).wait()
            same(r2d.at[s, j], rs2_recv.at[s, j, 1]).wait()
        wait_four(c, ld_sem)
        for k in range(2):
            g = accgu[s, k, rows_of(me), :] + r2gu[s, 0, k].astype(F32) + r2gu[s, 1, k].astype(F32)
            wngu[s, k], mvgu[s, 0, k], mvgu[s, 1, k] = adamw(wngu[s, k], mvgu[s, 0, k], mvgu[s, 1, k], g)
        g = accd[s, :, units_of(me)].T + r2d[s, 0].astype(F32) + r2d[s, 1].astype(F32)
        wnd[s], mvd[s, 0], mvd[s, 1] = adamw(wnd[s], mvd[s, 0], mvd[s, 1], g)
        for j, to in enumerate((right, left)):
            for k, w_out in enumerate((wg_out, wu_out)):
                for o in range(n):
                    send(wngu.at[s, k, :, part(o)], w_out.at[layer, rows_of(me), cols_of(o, i)],
                         ag1_send.at[s, j, 0], ag1_recv.at[s, j, 0], to)
            send(wnd.at[s], wd_out.at[layer, cols_of(me, i), :], ag1_send.at[s, j, 1], ag1_recv.at[s, j, 1], to)
        store_mvw(c)

    def gather_2(c):
        s, layer, i = where(c)
        for j, (w_out, owner, to) in enumerate(((wg_out, left, right), (wu_out, right, left))):
            same(wngu.at[s], ag1_recv.at[s, j, 0]).wait()
            same(wnd.at[s], ag1_recv.at[s, j, 1]).wait()
            for o in range(n):
                block = w_out.at[layer, rows_of(owner), cols_of(o, i)]
                send(block, block, ag2_send.at[s, j, 0], ag2_recv.at[s, j, 0], to)
            block = wd_out.at[layer, pl.ds(pl.multiple_of(owner * share + i * LANES + j * half, half), half), :]
            send(block, block, ag2_send.at[s, j, 1], ag2_recv.at[s, j, 1], to)

    def finish(c):
        s = c % 2
        for j in range(2):
            same(wngu.at[s], ag1_send.at[s, j, 0]).wait()
            same(wnd.at[s], ag1_send.at[s, j, 1]).wait()
            for sems in (ag2_send, ag2_recv):
                same(wngu.at[s, 0], sems.at[s, j, 0]).wait()
                same(wnd.at[s, :half], sems.at[s, j, 1]).wait()
        wait_four(c, st_sem)

    def rows_at(t):
        return pl.ds(pl.multiple_of(t * TILE, TILE), TILE)

    def copy_x(t):
        return pltpu.make_async_copy(x_in.at[0, rows_at(t)], x.at[rows_at(t)], tile_sem.at[0, t])

    def copy_dy(t):
        return pltpu.make_async_copy(dy_in.at[0, rows_at(t)], dy.at[rows_at(t)], tile_sem.at[1, t])

    load_w(0)
    for t in range(tiles):
        copy_x(t).start()
    for t in range(tiles):
        copy_dy(t).start()

    barrier = pltpu.get_barrier_semaphore()
    for to in (left, right):
        pl.semaphore_signal(barrier, inc=1, device_id={"dp": to}, device_id_type=pl.DeviceIdType.MESH)
    pl.semaphore_wait(barrier, 2)

    def begin(k):
        wait_w(k)

        @pl.when(k + 1 < 3 * chunks)
        def _():
            load_w(k + 1)

    @pl.loop(0, chunks)
    def _(i):
        begin(i)
        slot = i % 2

        @pl.loop(0, tiles)
        def _(t):
            r = rows_at(t)

            @pl.when(i == 0)
            def _():
                copy_x(t).wait()
                a[r] = normed(x[r])
                acc[r] = jnp.zeros((TILE, d_model), F32)

            at = a[r]
            gate, up = nn(at, wg[slot]), nn(at, wu[slot])
            hidden = (gate * jax.nn.sigmoid(gate) * up).astype(BF16)
            acc[r] += nn(hidden, wd[slot])

            @pl.when(i == chunks - 1)
            def _():
                h1[r] = x[r] + acc[r].astype(BF16)

    def backward(k, i, states, last):
        c = k - chunks
        s, slot = c % 2, k % 2
        begin(k)

        @pl.loop(0, tiles)
        def _(t):
            r = rows_at(t)

            @pl.when(i == 0)
            def _():
                if last:
                    copy_dy(t).wait()
                    acc[r] = jnp.zeros((TILE, d_model), F32)
                a[r] = normed(states[r])

            at, dyt = a[r], dy[r]
            gate, up = nn(at, wg[slot]), nn(at, wu[slot])
            by_hidden = nt(dyt, wd[slot]).astype(BF16).astype(F32)
            sigmoid = jax.nn.sigmoid(gate)
            silu = gate * sigmoid
            hidden = (silu * up).astype(BF16)
            by_up = (by_hidden * silu).astype(BF16)
            by_gate = (by_hidden * up * (sigmoid + silu * (1 - sigmoid))).astype(BF16)
            new = t == 0
            accd[s] = jnp.where(new, 0.0, accd[s]) + tn(dyt, hidden)
            accgu[s, 0] = jnp.where(new, 0.0, accgu[s, 0]) + tn(at, by_gate)
            accgu[s, 1] = jnp.where(new, 0.0, accgu[s, 1]) + tn(at, by_up)
            if last:
                acc[r] += nt(by_gate, wg[slot]) + nt(by_up, wu[slot])

                @pl.when(i == chunks - 1)
                def _():
                    dy[r] = dyt + normed_back(states[r], acc[r].astype(BF16).astype(F32))

            @pl.when((t == tiles * 3 // 8) & (c >= 2))
            def _():
                gather_2(c - 2)

            @pl.when((t == tiles * 5 // 8) & (c >= 1))
            def _():
                sum_2(c - 1)

        sum_1(c)

        @pl.when(c >= 2)
        def _():
            finish(c - 2)

        load_mvw(c)

        @pl.when(c >= 1)
        def _():
            sum_3(c - 1)

    @pl.loop(0, chunks)
    def _(i):
        backward(chunks + i, i, h1, True)

    @pl.loop(0, chunks)
    def _(i):
        backward(2 * chunks + i, i, x, False)

    end = 2 * chunks - 1
    sum_2(end)
    gather_2(end - 1)
    sum_3(end)
    finish(end - 1)
    gather_2(end)
    finish(end)


def solution(mesh):
    n = mesh.shape["dp"]

    def step(x, dy, *arrays):
        weights, moments = arrays[:3], arrays[3:]
        tokens, d_model = x.shape[1:]
        ff = weights[0].shape[2]
        chunk, rows, half = n * LANES, d_model // n, LANES // 2
        out = lambda like, dtype: jax.ShapeDtypeStruct(like.shape, dtype)
        vmem, dma = pltpu.VMEM, pltpu.SemaphoreType.DMA
        return pl.pallas_call(
            functools.partial(kernel, n),
            out_shape=[out(w, BF16) for w in weights] + [out(m, F32) for m in moments],
            in_specs=[pl.BlockSpec(memory_space=pl.ANY)] * 11,
            out_specs=[pl.BlockSpec(memory_space=pl.ANY)] * 9,
            scratch_shapes=[
                vmem((tokens, d_model), BF16),
                vmem((tokens, d_model), BF16),
                vmem((tokens, d_model), BF16),
                vmem((tokens, d_model), BF16),
                vmem((tokens, d_model), F32),
                vmem((2, 2, d_model, chunk), F32),
                vmem((2, d_model, chunk), F32),
                vmem((2, d_model, chunk), BF16),
                vmem((2, d_model, chunk), BF16),
                vmem((2, chunk, d_model), BF16),
                vmem((2, rows, chunk), BF16),
                vmem((2, half, d_model), BF16),
                vmem((2, 2, rows, chunk), BF16),
                vmem((2, 2, half, d_model), BF16),
                vmem((2, 2, rows, chunk), BF16),
                vmem((2, LANES, d_model), BF16),
                vmem((2, 2, 2, rows, chunk), BF16),
                vmem((2, 2, LANES, d_model), BF16),
                vmem((2, 2, rows, chunk), BF16),
                vmem((2, LANES, d_model), BF16),
                vmem((2, 2, 2, rows, chunk), F32),
                vmem((2, 2, LANES, d_model), F32),
                dma((2, tokens // TILE)),
                dma((2, 3)),
                dma((2, 4)),
                dma((2, 4)),
                dma((2, 2)),
                dma((2, 2, 2)),
                dma((2, 2)),
                dma((2, 2, 2)),
                dma((2, 2, 2)),
                dma((2, 2, 2)),
                dma((2, 2, 2)),
                dma((2, 2, 2)),
            ],
            compiler_params=pltpu.CompilerParams(
                collective_id=0, has_side_effects=True, vmem_limit_bytes=67043328
            ),
            name="train_step",
        )(x, dy, *arrays)

    tokens, whole = P(("rep", "dp"), None, None), P(None, None, None)
    shares = [P(None, "dp", None)] * 6
    return jax.shard_map(
        step,
        mesh=mesh,
        in_specs=(tokens, tokens, whole, whole, whole, *shares),
        out_specs=tuple([P("rep", None, None)] * 3 + [P("rep", "dp", None)] * 6),
        check_vma=False,
    )
```

```python
import functools

import jax
import jax.numpy as jnp
from jax import lax
from jax.experimental import pallas as pl
from jax.experimental.pallas import tpu as pltpu
from jax.sharding import PartitionSpec as P

F32, BF16 = jnp.float32, jnp.bfloat16
TILE = 1024
LANES = 128
HALVES = 2


def nn(a, b):
    return lax.dot_general(a, b, (((1,), (0,)), ((), ())), preferred_element_type=F32)


def nt(a, b):
    return lax.dot_general(a, b, (((1,), (1,)), ((), ())), preferred_element_type=F32)


def tn(a, b):
    return lax.dot_general(a, b, (((0,), (0,)), ((), ())), preferred_element_type=F32)


def normed(h):
    wide = h.astype(F32)
    scale = lax.rsqrt(jnp.mean(wide * wide, -1, keepdims=True) + 1e-6)
    return (wide * scale).astype(BF16)


def normed_back(h, by_a):
    wide = h.astype(F32)
    scale = lax.rsqrt(jnp.mean(wide * wide, -1, keepdims=True) + 1e-6)
    along = jnp.mean(by_a * wide, -1, keepdims=True)
    return (scale * by_a - wide * (scale * scale * scale * along)).astype(BF16)


def kernel(
    n,
    x_in, dy_in, wg_in, wu_in, wd_in, mg_in, mu_in, md_in, vg_in, vu_in, vd_in,
    wg_out, wu_out, wd_out, mg_out, mu_out, md_out, vg_out, vu_out, vd_out,
    x, h1, dy, a, acc, accgu, accd, wg, wu, wd,
    s1gu, s1d, r1gu, r1d, s2gu, s2d, r2gu, r2d, wngu, wnd, mvgu, mvd,
    tile_sem, w_sem, ld_sem, st_sem,
    rs1_send, rs1_recv, rs2_send, rs2_recv, ag1_send, ag1_recv, ag2_send, ag2_recv,
):
    tokens, d_model = x.shape
    ff = wg_in.shape[2]
    tiles = tokens // TILE
    share = ff // n
    chunks = share // LANES
    owners = n // HALVES
    width = owners * LANES
    units = chunks * HALVES
    rows = d_model // n
    half = LANES // 2

    me = lax.axis_index("dp")
    right, left, far = (lax.rem(me + k, n) for k in (1, n - 1, n // 2))

    def cols_of(owner, i):
        return pl.ds(pl.multiple_of(owner * share + i * LANES, LANES), LANES)

    def rows_of(owner):
        return pl.ds(pl.multiple_of(owner * rows, rows), rows)

    def units_of(owner):
        return pl.ds(pl.multiple_of(owner * LANES, LANES), LANES)

    def same(ref, sem):
        return pltpu.make_async_copy(ref, ref, sem)

    def part(owner):
        return slice(owner * LANES, (owner + 1) * LANES)

    def load_w(k):
        slot, layer, i = k % 2, (k // chunks) % 2, k % chunks
        for o in range(n):
            pltpu.make_async_copy(wg_in.at[layer, :, cols_of(o, i)], wg.at[slot, :, part(o)], w_sem.at[slot, 0]).start()
            pltpu.make_async_copy(wu_in.at[layer, :, cols_of(o, i)], wu.at[slot, :, part(o)], w_sem.at[slot, 1]).start()
            pltpu.make_async_copy(wd_in.at[layer, cols_of(o, i), :], wd.at[slot, part(o), :], w_sem.at[slot, 2]).start()

    def wait_w(k):
        slot = k % 2
        for j, ref in enumerate((wg, wu, wd)):
            same(ref.at[slot], w_sem.at[slot, j]).wait()

    def where(u):
        return u % HALVES, 1 - u // units, (u // HALVES) % chunks

    def second(h, do):
        pl.when(h == HALVES - 1)(do)

    def load_mvw(u):
        h, layer, i = where(u)
        for q in range(owners):
            cols = cols_of(h * owners + q, i)
            for j, (m_in, v_in, w_in) in enumerate(((mg_in, vg_in, wg_in), (mu_in, vu_in, wu_in))):
                pltpu.make_async_copy(m_in.at[layer, :, cols], mvgu.at[h, 0, j, :, part(q)], ld_sem.at[h, 0]).start()
                pltpu.make_async_copy(v_in.at[layer, :, cols], mvgu.at[h, 1, j, :, part(q)], ld_sem.at[h, 0]).start()
                pltpu.make_async_copy(w_in.at[layer, rows_of(me), cols], wngu.at[h, j, :, part(q)], ld_sem.at[h, 1]).start()

        def down():
            mine = pl.ds(pl.multiple_of(i * LANES, LANES), LANES)
            pltpu.make_async_copy(md_in.at[layer, mine, :], mvd.at[0], ld_sem.at[0, 2]).start()
            pltpu.make_async_copy(vd_in.at[layer, mine, :], mvd.at[1], ld_sem.at[0, 2]).start()
            pltpu.make_async_copy(wd_in.at[layer, cols_of(me, i), :], wnd, ld_sem.at[1, 2]).start()

        second(h, down)

    def wait_mvw(u, sem):
        h = u % HALVES
        same(mvgu.at[h], sem.at[h, 0]).wait()
        same(wngu.at[h], sem.at[h, 1]).wait()

        def down():
            same(mvd, sem.at[0, 2]).wait()
            same(wnd, sem.at[1, 2]).wait()

        second(h, down)

    def store_mvw(u):
        h, layer, i = where(u)
        for q in range(owners):
            cols = cols_of(h * owners + q, i)
            for j, (m_out, v_out, w_out) in enumerate(((mg_out, vg_out, wg_out), (mu_out, vu_out, wu_out))):
                pltpu.make_async_copy(mvgu.at[h, 0, j, :, part(q)], m_out.at[layer, :, cols], st_sem.at[h, 0]).start()
                pltpu.make_async_copy(mvgu.at[h, 1, j, :, part(q)], v_out.at[layer, :, cols], st_sem.at[h, 0]).start()
                pltpu.make_async_copy(wngu.at[h, j, :, part(q)], w_out.at[layer, rows_of(me), cols], st_sem.at[h, 1]).start()

        def down():
            mine = pl.ds(pl.multiple_of(i * LANES, LANES), LANES)
            pltpu.make_async_copy(mvd.at[0], md_out.at[layer, mine, :], st_sem.at[0, 2]).start()
            pltpu.make_async_copy(mvd.at[1], vd_out.at[layer, mine, :], st_sem.at[0, 2]).start()
            pltpu.make_async_copy(wnd, wd_out.at[layer, cols_of(me, i), :], st_sem.at[1, 2]).start()

        second(h, down)

    def send(src, dst, send_sem, recv_sem, to):
        pltpu.make_async_remote_copy(
            src_ref=src, dst_ref=dst, send_sem=send_sem, recv_sem=recv_sem,
            device_id={"dp": to}, device_id_type=pl.DeviceIdType.MESH,
        ).start()

    def sum_1(u):
        h, _, i = where(u)
        for j, to in enumerate((right, left)):
            s1gu[j] = accgu[h, j, rows_of(far), :].astype(BF16)
            send(s1gu.at[j], r1gu.at[h, j], rs1_send.at[j, 0], rs1_recv.at[h, j], to)

        def down():
            block = accd[i % 2, :, units_of(far)].T
            for j, to in enumerate((right, left)):
                s1d[j] = block[j * half : (j + 1) * half].astype(BF16)
                send(s1d.at[j], r1d.at[j], rs1_send.at[j, 1], rs1_recv.at[2, j], to)

        second(h, down)

    def sum_2(u):
        h, _, i = where(u)
        for j, to in enumerate((right, left)):
            same(s1gu.at[j], rs1_send.at[j, 0]).wait()
            same(r1gu.at[h, j], rs1_recv.at[h, j]).wait()
            for k in range(2):
                total = accgu[h, k, rows_of(to), :]
                if k == j:
                    total += r1gu[h, j].astype(F32)
                s2gu[j, k] = total.astype(BF16)
            send(s2gu.at[j], r2gu.at[h, j], rs2_send.at[j, 0], rs2_recv.at[h, j], to)

        def down():
            for j, to in enumerate((right, left)):
                same(s1d.at[j], rs1_send.at[j, 1]).wait()
                same(r1d.at[j], rs1_recv.at[2, j]).wait()
                block = accd[i % 2, :, units_of(to)].T
                for k in range(2):
                    total = block[k * half : (k + 1) * half]
                    if k == j:
                        total += r1d[j].astype(F32)
                    s2d[j, k * half : (k + 1) * half] = total.astype(BF16)
                send(s2d.at[j], r2d.at[j], rs2_send.at[j, 1], rs2_recv.at[2, j], to)

        second(h, down)

    def adamw(w, m, v, g):
        g = g.astype(BF16).astype(F32)
        m = 0.9 * m + 0.1 * g
        v = 0.95 * v + 0.05 * g * g
        w = w.astype(F32)
        return (w - 0.02 * (m * lax.rsqrt(v + 1e-8) + 0.1 * w)).astype(BF16), m, v

    def sum_3(u):
        h, layer, i = where(u)
        wait_mvw(u, ld_sem)
        for j in range(2):
            same(s2gu.at[j], rs2_send.at[j, 0]).wait()
            same(r2gu.at[h, j], rs2_recv.at[h, j]).wait()
        for k in range(2):
            g = accgu[h, k, rows_of(me), :] + r2gu[h, 0, k].astype(F32) + r2gu[h, 1, k].astype(F32)
            wngu[h, k], mvgu[h, 0, k], mvgu[h, 1, k] = adamw(wngu[h, k], mvgu[h, 0, k], mvgu[h, 1, k], g)
        for j, to in enumerate((right, left)):
            for k, w_out in enumerate((wg_out, wu_out)):
                for q in range(owners):
                    send(wngu.at[h, k, :, part(q)], w_out.at[layer, rows_of(me), cols_of(h * owners + q, i)],
                         ag1_send.at[h, j], ag1_recv.at[h, j], to)

        def down():
            for j in range(2):
                same(s2d.at[j], rs2_send.at[j, 1]).wait()
                same(r2d.at[j], rs2_recv.at[2, j]).wait()
            g = accd[i % 2, :, units_of(me)].T + r2d[0].astype(F32) + r2d[1].astype(F32)
            wnd[...], mvd[0], mvd[1] = adamw(wnd[...], mvd[0], mvd[1], g)
            for j, to in enumerate((right, left)):
                send(wnd, wd_out.at[layer, cols_of(me, i), :], ag1_send.at[2, j], ag1_recv.at[2, j], to)

        second(h, down)
        store_mvw(u)

    def gather_2(u):
        h, layer, i = where(u)
        ways = tuple(enumerate(((wg_out, left, right), (wu_out, right, left))))
        for j, (w_out, owner, to) in ways:
            same(wngu.at[h], ag1_recv.at[h, j]).wait()
            for q in range(owners):
                block = w_out.at[layer, rows_of(owner), cols_of(h * owners + q, i)]
                send(block, block, ag2_send.at[h, j], ag2_recv.at[h, j], to)

        def down():
            for j, (_, owner, to) in ways:
                same(wnd, ag1_recv.at[2, j]).wait()
                block = wd_out.at[layer, pl.ds(pl.multiple_of(owner * share + i * LANES + j * half, half), half), :]
                send(block, block, ag2_send.at[2, j], ag2_recv.at[2, j], to)

        second(h, down)

    def finish(u):
        h = u % HALVES
        for j in range(2):
            same(wngu.at[h], ag1_send.at[h, j]).wait()
            for sems in (ag2_send, ag2_recv):
                same(wngu.at[h, 0], sems.at[h, j]).wait()

        def down():
            for j in range(2):
                same(wnd, ag1_send.at[2, j]).wait()
                for sems in (ag2_send, ag2_recv):
                    same(wnd.at[:half], sems.at[2, j]).wait()

        second(h, down)
        wait_mvw(u, st_sem)

    def rows_at(t):
        return pl.ds(pl.multiple_of(t * TILE, TILE), TILE)

    def copy_x(t):
        return pltpu.make_async_copy(x_in.at[0, rows_at(t)], x.at[rows_at(t)], tile_sem.at[0, t])

    def copy_dy(t):
        return pltpu.make_async_copy(dy_in.at[0, rows_at(t)], dy.at[rows_at(t)], tile_sem.at[1, t])

    load_w(0)
    for t in range(tiles):
        copy_x(t).start()
    for t in range(tiles):
        copy_dy(t).start()

    barrier = pltpu.get_barrier_semaphore()
    for to in (left, right):
        pl.semaphore_signal(barrier, inc=1, device_id={"dp": to}, device_id_type=pl.DeviceIdType.MESH)
    pl.semaphore_wait(barrier, 2)

    def begin(k):
        wait_w(k)

        @pl.when(k + 1 < 3 * chunks)
        def _():
            load_w(k + 1)

    @pl.loop(0, chunks)
    def _(i):
        begin(i)
        slot = i % 2

        @pl.loop(0, tiles)
        def _(t):
            r = rows_at(t)

            @pl.when(i == 0)
            def _():
                copy_x(t).wait()
                a[r] = normed(x[r])
                acc[r] = jnp.zeros((TILE, d_model), F32)

            at = a[r]
            gate, up = nn(at, wg[slot]), nn(at, wu[slot])
            hidden = (gate * jax.nn.sigmoid(gate) * up).astype(BF16)
            acc[r] += nn(hidden, wd[slot])

            @pl.when(i == chunks - 1)
            def _():
                h1[r] = x[r] + acc[r].astype(BF16)

    def backward(u, states, last):
        h, _, i = where(u)
        k = chunks + u // HALVES
        slot = k % 2
        first = u % units == 0
        hidden_units = pl.ds(pl.multiple_of(h * width, width), width)

        @pl.when(h == 0)
        def _():
            begin(k)

        @pl.loop(0, tiles)
        def _(t):
            r = rows_at(t)

            @pl.when(first)
            def _():
                if last:
                    copy_dy(t).wait()
                    acc[r] = jnp.zeros((TILE, d_model), F32)
                a[r] = normed(states[r])

            at, dyt = a[r], dy[r]
            wgt, wut = wg[slot, :, hidden_units], wu[slot, :, hidden_units]
            gate, up = nn(at, wgt), nn(at, wut)
            by_hidden = nt(dyt, wd[slot, hidden_units, :]).astype(BF16).astype(F32)
            sigmoid = jax.nn.sigmoid(gate)
            silu = gate * sigmoid
            hidden = (silu * up).astype(BF16)
            by_up = (by_hidden * silu).astype(BF16)
            by_gate = (by_hidden * up * (sigmoid + silu * (1 - sigmoid))).astype(BF16)
            new = t == 0
            accd[i % 2, :, hidden_units] = jnp.where(new, 0.0, accd[i % 2, :, hidden_units]) + tn(dyt, hidden)
            accgu[h, 0] = jnp.where(new, 0.0, accgu[h, 0]) + tn(at, by_gate)
            accgu[h, 1] = jnp.where(new, 0.0, accgu[h, 1]) + tn(at, by_up)
            if last:
                acc[r] += nt(by_gate, wgt) + nt(by_up, wut)

                @pl.when(u == units - 1)
                def _():
                    dy[r] = dyt + normed_back(states[r], acc[r].astype(BF16).astype(F32))

            @pl.when(t == 0)
            def _():
                @pl.when(u >= 3)
                def _():
                    finish(u - 3)

                @pl.when(u >= 1)
                def _():
                    sum_2(u - 1)
                    load_mvw(u - 1)

            @pl.when((t == tiles - 2) & (u >= 2))
            def _():
                gather_2(u - 2)

        sum_1(u)

        @pl.when(u >= 1)
        def _():
            sum_3(u - 1)

    @pl.loop(0, units)
    def _(u):
        backward(u, h1, True)

    @pl.loop(units, 2 * units)
    def _(u):
        backward(u, x, False)

    end = 2 * units - 1
    finish(end - 2)
    sum_2(end)
    load_mvw(end)
    gather_2(end - 1)
    sum_3(end)
    finish(end - 1)
    gather_2(end)
    finish(end)


def pieces_of(shape, dtype):
    layers, height, width = shape
    cut = max(1, height * width * jnp.dtype(dtype).itemsize // 1300000)
    while height % (cut * 8):
        cut -= 1
    return [(l, slice(k * height // cut, (k + 1) * height // cut)) for l in range(layers) for k in range(cut)]


def copies(*refs):
    count = (len(refs) - 2) // 3
    source, target, held = (refs[k * count : (k + 1) * count] for k in range(3))
    in_sem, out_sem = refs[-2:]
    places = [(k, *at) for k, ref in enumerate(source) for at in pieces_of(ref.shape, ref.dtype)]
    way_in = [pltpu.make_async_copy(source[k].at[l, s], held[k].at[l, s], in_sem.at[p]) for p, (k, l, s) in enumerate(places)]
    way_out = [pltpu.make_async_copy(held[k].at[l, s], target[k].at[l, s], out_sem.at[p]) for p, (k, l, s) in enumerate(places)]
    for copy in way_in:
        copy.start()
    for p, copy in enumerate(way_out):
        way_in[p].wait()
        copy.start()
    for copy in way_out:
        copy.wait()


def solution(mesh):
    n = mesh.shape["dp"]
    most = 67043328

    def step(x, dy, *arrays):
        weights, moments = arrays[:3], arrays[3:]
        tokens, d_model = x.shape[1:]
        chunk, rows, half = n * LANES, d_model // n, LANES // 2
        width = chunk // HALVES
        shapes = [jax.ShapeDtypeStruct(w.shape, BF16) for w in weights] + [jax.ShapeDtypeStruct(m.shape, F32) for m in moments]
        vmem, dma = pltpu.VMEM, pltpu.SemaphoreType.DMA
        anywhere = pl.BlockSpec(memory_space=pl.ANY)
        new = pl.pallas_call(
            functools.partial(kernel, n),
            out_shape=shapes,
            in_specs=[anywhere] * 11,
            out_specs=[anywhere] * 9,
            scratch_shapes=[
                vmem((tokens, d_model), BF16),
                vmem((tokens, d_model), BF16),
                vmem((tokens, d_model), BF16),
                vmem((tokens, d_model), BF16),
                vmem((tokens, d_model), F32),
                vmem((HALVES, 2, d_model, width), F32),
                vmem((2, d_model, chunk), F32),
                vmem((2, d_model, chunk), BF16),
                vmem((2, d_model, chunk), BF16),
                vmem((2, chunk, d_model), BF16),
                vmem((2, rows, width), BF16),
                vmem((2, half, d_model), BF16),
                vmem((HALVES, 2, rows, width), BF16),
                vmem((2, half, d_model), BF16),
                vmem((2, 2, rows, width), BF16),
                vmem((2, LANES, d_model), BF16),
                vmem((HALVES, 2, 2, rows, width), BF16),
                vmem((2, LANES, d_model), BF16),
                vmem((HALVES, 2, rows, width), BF16),
                vmem((LANES, d_model), BF16),
                vmem((HALVES, 2, 2, rows, width), F32),
                vmem((2, LANES, d_model), F32),
                dma((2, tokens // TILE)),
                dma((2, 3)),
                dma((2, 3)),
                dma((2, 3)),
                dma((2, 2)),
                dma((HALVES + 1, 2)),
                dma((2, 2)),
                dma((HALVES + 1, 2)),
                dma((HALVES + 1, 2)),
                dma((HALVES + 1, 2)),
                dma((HALVES + 1, 2)),
                dma((HALVES + 1, 2)),
            ],
            compiler_params=pltpu.CompilerParams(collective_id=0, has_side_effects=True, vmem_limit_bytes=most),
            name="train_step",
        )(x, dy, *arrays)
        places = sum(len(pieces_of(s.shape, s.dtype)) for s in shapes)
        return pl.pallas_call(
            copies,
            out_shape=shapes,
            in_specs=[anywhere] * 9,
            out_specs=[anywhere] * 9,
            scratch_shapes=[vmem(s.shape, s.dtype) for s in shapes] + [dma((places,)), dma((places,))],
            compiler_params=pltpu.CompilerParams(vmem_limit_bytes=most),
            name="results",
        )(*new)

    tokens, whole = P(("rep", "dp"), None, None), P(None, None, None)
    shares = [P(None, "dp", None)] * 6
    return jax.shard_map(
        step,
        mesh=mesh,
        in_specs=(tokens, tokens, whole, whole, whole, *shares),
        out_specs=tuple([P("rep", None, None)] * 3 + [P("rep", "dp", None)] * 6),
        check_vma=False,
    )
```

```python
import functools

import jax
import jax.numpy as jnp
from jax import lax
from jax.experimental import pallas as pl
from jax.experimental.pallas import tpu as pltpu
from jax.sharding import PartitionSpec as P

F32, BF16 = jnp.float32, jnp.bfloat16
TILE = 1024
LANES = 128
HALVES = 2


def nn(a, b):
    return lax.dot_general(a, b, (((1,), (0,)), ((), ())), preferred_element_type=F32)


def nt(a, b):
    return lax.dot_general(a, b, (((1,), (1,)), ((), ())), preferred_element_type=F32)


def tn(a, b):
    return lax.dot_general(a, b, (((0,), (0,)), ((), ())), preferred_element_type=F32)


def normed(h):
    wide = h.astype(F32)
    scale = lax.rsqrt(jnp.mean(wide * wide, -1, keepdims=True) + 1e-6)
    return (wide * scale).astype(BF16)


def normed_back(h, by_a):
    wide = h.astype(F32)
    scale = lax.rsqrt(jnp.mean(wide * wide, -1, keepdims=True) + 1e-6)
    along = jnp.mean(by_a * wide, -1, keepdims=True)
    return (scale * by_a - wide * (scale * scale * scale * along)).astype(BF16)


def kernel(
    n,
    x_in, dy_in, wg_in, wu_in, wd_in, mg_in, mu_in, md_in, vg_in, vu_in, vd_in,
    wg_out, wu_out, wd_out, mg_out, mu_out, md_out, vg_out, vu_out, vd_out,
    x, h1, dy, a, acc, accgu, accd, wgu, wd,
    s1gu, s1d, r1gu, r1d, s2gu, s2d, r2gu, r2d, wngu, wnd, mvgu, mvd,
    tile_sem, w_sem, ld_sem, st_sem,
    rs1_send, rs1_recv, rs2_send, rs2_recv, ag1_send, ag1_recv, ag2_send, ag2_recv,
):
    tokens, d_model = x.shape
    ff = wg_in.shape[2]
    tiles = tokens // TILE
    share = ff // n
    chunks = share // LANES
    owners = n // HALVES
    width = owners * LANES
    units = chunks * HALVES
    rows = d_model // n
    half = LANES // 2

    me = lax.axis_index("dp")
    right, left, far = (lax.rem(me + k, n) for k in (1, n - 1, n // 2))

    def cols_of(owner, i):
        return pl.ds(pl.multiple_of(owner * share + i * LANES, LANES), LANES)

    def rows_of(owner):
        return pl.ds(pl.multiple_of(owner * rows, rows), rows)

    def units_of(owner):
        return pl.ds(pl.multiple_of(owner * LANES, LANES), LANES)

    def same(ref, sem):
        return pltpu.make_async_copy(ref, ref, sem)

    def part(owner):
        return slice(owner * LANES, (owner + 1) * LANES)

    def lanes_of(k):
        return slice(k * width, (k + 1) * width)

    def load_w(k):
        slot, layer, i = k % 2, (k // chunks) % 2, k % chunks
        for o in range(n):
            for k, w_in in enumerate((wg_in, wu_in)):
                place = part((o // owners * 2 + k) * owners + o % owners)
                pltpu.make_async_copy(w_in.at[layer, :, cols_of(o, i)], wgu.at[slot, :, place], w_sem.at[slot, 0]).start()
            pltpu.make_async_copy(wd_in.at[layer, cols_of(o, i), :], wd.at[slot, part(o), :], w_sem.at[slot, 1]).start()

    def wait_w(k):
        slot = k % 2
        for j, ref in enumerate((wgu, wd)):
            same(ref.at[slot], w_sem.at[slot, j]).wait()

    def where(u):
        return u % HALVES, 1 - u // units, (u // HALVES) % chunks

    def second(h, do):
        pl.when(h == HALVES - 1)(do)

    def load_mvw(u):
        h, layer, i = where(u)
        for q in range(owners):
            cols = cols_of(h * owners + q, i)
            for j, (m_in, v_in, w_in) in enumerate(((mg_in, vg_in, wg_in), (mu_in, vu_in, wu_in))):
                pltpu.make_async_copy(m_in.at[layer, :, cols], mvgu.at[h, 0, j, :, part(q)], ld_sem.at[h, 0]).start()
                pltpu.make_async_copy(v_in.at[layer, :, cols], mvgu.at[h, 1, j, :, part(q)], ld_sem.at[h, 0]).start()
                pltpu.make_async_copy(w_in.at[layer, rows_of(me), cols], wngu.at[h, j, :, part(q)], ld_sem.at[h, 1]).start()

        def down():
            mine = pl.ds(pl.multiple_of(i * LANES, LANES), LANES)
            pltpu.make_async_copy(md_in.at[layer, mine, :], mvd.at[0], ld_sem.at[0, 2]).start()
            pltpu.make_async_copy(vd_in.at[layer, mine, :], mvd.at[1], ld_sem.at[0, 2]).start()
            pltpu.make_async_copy(wd_in.at[layer, cols_of(me, i), :], wnd, ld_sem.at[1, 2]).start()

        second(h, down)

    def wait_mvw(u, sem):
        h = u % HALVES
        same(mvgu.at[h], sem.at[h, 0]).wait()
        same(wngu.at[h], sem.at[h, 1]).wait()

        def down():
            same(mvd, sem.at[0, 2]).wait()
            same(wnd, sem.at[1, 2]).wait()

        second(h, down)

    def store_mvw(u):
        h, layer, i = where(u)
        for q in range(owners):
            cols = cols_of(h * owners + q, i)
            for j, (m_out, v_out, w_out) in enumerate(((mg_out, vg_out, wg_out), (mu_out, vu_out, wu_out))):
                pltpu.make_async_copy(mvgu.at[h, 0, j, :, part(q)], m_out.at[layer, :, cols], st_sem.at[h, 0]).start()
                pltpu.make_async_copy(mvgu.at[h, 1, j, :, part(q)], v_out.at[layer, :, cols], st_sem.at[h, 0]).start()
                pltpu.make_async_copy(wngu.at[h, j, :, part(q)], w_out.at[layer, rows_of(me), cols], st_sem.at[h, 1]).start()

        def down():
            mine = pl.ds(pl.multiple_of(i * LANES, LANES), LANES)
            pltpu.make_async_copy(mvd.at[0], md_out.at[layer, mine, :], st_sem.at[0, 2]).start()
            pltpu.make_async_copy(mvd.at[1], vd_out.at[layer, mine, :], st_sem.at[0, 2]).start()
            pltpu.make_async_copy(wnd, wd_out.at[layer, cols_of(me, i), :], st_sem.at[1, 2]).start()

        second(h, down)

    def send(src, dst, send_sem, recv_sem, to):
        pltpu.make_async_remote_copy(
            src_ref=src, dst_ref=dst, send_sem=send_sem, recv_sem=recv_sem,
            device_id={"dp": to}, device_id_type=pl.DeviceIdType.MESH,
        ).start()

    def sum_1(u):
        h, _, i = where(u)
        for j, to in enumerate((right, left)):
            s1gu[j] = accgu[h, rows_of(far), lanes_of(j)].astype(BF16)
            send(s1gu.at[j], r1gu.at[h, j], rs1_send.at[j, 0], rs1_recv.at[h, j], to)

        def down():
            block = accd[i % 2, :, units_of(far)].T
            for j, to in enumerate((right, left)):
                s1d[j] = block[j * half : (j + 1) * half].astype(BF16)
                send(s1d.at[j], r1d.at[j], rs1_send.at[j, 1], rs1_recv.at[2, j], to)

        second(h, down)

    def sum_2(u):
        h, _, i = where(u)
        for j, to in enumerate((right, left)):
            same(s1gu.at[j], rs1_send.at[j, 0]).wait()
            same(r1gu.at[h, j], rs1_recv.at[h, j]).wait()
            for k in range(2):
                total = accgu[h, rows_of(to), lanes_of(k)]
                if k == j:
                    total += r1gu[h, j].astype(F32)
                s2gu[j, k] = total.astype(BF16)
            send(s2gu.at[j], r2gu.at[h, j], rs2_send.at[j, 0], rs2_recv.at[h, j], to)

        def down():
            for j, to in enumerate((right, left)):
                same(s1d.at[j], rs1_send.at[j, 1]).wait()
                same(r1d.at[j], rs1_recv.at[2, j]).wait()
                block = accd[i % 2, :, units_of(to)].T
                for k in range(2):
                    total = block[k * half : (k + 1) * half]
                    if k == j:
                        total += r1d[j].astype(F32)
                    s2d[j, k * half : (k + 1) * half] = total.astype(BF16)
                send(s2d.at[j], r2d.at[j], rs2_send.at[j, 1], rs2_recv.at[2, j], to)

        second(h, down)

    def adamw(w, m, v, g):
        g = g.astype(BF16).astype(F32)
        m = 0.9 * m + 0.1 * g
        v = 0.95 * v + 0.05 * g * g
        w = w.astype(F32)
        return (w - 0.02 * (m * lax.rsqrt(v + 1e-8) + 0.1 * w)).astype(BF16), m, v

    def sum_3(u):
        h, layer, i = where(u)
        wait_mvw(u, ld_sem)
        for j in range(2):
            same(s2gu.at[j], rs2_send.at[j, 0]).wait()
            same(r2gu.at[h, j], rs2_recv.at[h, j]).wait()
        for k in range(2):
            g = accgu[h, rows_of(me), lanes_of(k)] + r2gu[h, 0, k].astype(F32) + r2gu[h, 1, k].astype(F32)
            wngu[h, k], mvgu[h, 0, k], mvgu[h, 1, k] = adamw(wngu[h, k], mvgu[h, 0, k], mvgu[h, 1, k], g)
        for j, to in enumerate((right, left)):
            for k, w_out in enumerate((wg_out, wu_out)):
                for q in range(owners):
                    send(wngu.at[h, k, :, part(q)], w_out.at[layer, rows_of(me), cols_of(h * owners + q, i)],
                         ag1_send.at[h, j], ag1_recv.at[h, j], to)

        def down():
            for j in range(2):
                same(s2d.at[j], rs2_send.at[j, 1]).wait()
                same(r2d.at[j], rs2_recv.at[2, j]).wait()
            g = accd[i % 2, :, units_of(me)].T + r2d[0].astype(F32) + r2d[1].astype(F32)
            wnd[...], mvd[0], mvd[1] = adamw(wnd[...], mvd[0], mvd[1], g)
            for j, to in enumerate((right, left)):
                send(wnd, wd_out.at[layer, cols_of(me, i), :], ag1_send.at[2, j], ag1_recv.at[2, j], to)

        second(h, down)
        store_mvw(u)

    def gather_2(u):
        h, layer, i = where(u)
        ways = tuple(enumerate(((wg_out, left, right), (wu_out, right, left))))
        for j, (w_out, owner, to) in ways:
            same(wngu.at[h], ag1_recv.at[h, j]).wait()
            for q in range(owners):
                block = w_out.at[layer, rows_of(owner), cols_of(h * owners + q, i)]
                send(block, block, ag2_send.at[h, j], ag2_recv.at[h, j], to)

        def down():
            for j, (_, owner, to) in ways:
                same(wnd, ag1_recv.at[2, j]).wait()
                block = wd_out.at[layer, pl.ds(pl.multiple_of(owner * share + i * LANES + j * half, half), half), :]
                send(block, block, ag2_send.at[2, j], ag2_recv.at[2, j], to)

        second(h, down)

    def finish(u):
        h = u % HALVES
        for j in range(2):
            same(wngu.at[h], ag1_send.at[h, j]).wait()
            for sems in (ag2_send, ag2_recv):
                same(wngu.at[h, 0], sems.at[h, j]).wait()

        def down():
            for j in range(2):
                same(wnd, ag1_send.at[2, j]).wait()
                for sems in (ag2_send, ag2_recv):
                    same(wnd.at[:half], sems.at[2, j]).wait()

        second(h, down)
        wait_mvw(u, st_sem)

    def rows_at(t, tile=TILE):
        return pl.ds(pl.multiple_of(t * tile, tile), tile)

    def copy_x(t):
        r = rows_at(t, 2 * TILE)
        return pltpu.make_async_copy(x_in.at[0, r], x.at[r], tile_sem.at[0, t])

    def copy_dy(t):
        return pltpu.make_async_copy(dy_in.at[0, rows_at(t)], dy.at[rows_at(t)], tile_sem.at[1, t])

    copy_x(0).start()
    load_w(0)
    barrier = pltpu.get_barrier_semaphore()
    for to in (left, right):
        pl.semaphore_signal(barrier, inc=1, device_id={"dp": to}, device_id_type=pl.DeviceIdType.MESH)

    def begin(k):
        wait_w(k)

        @pl.when(k + 1 < 3 * chunks)
        def _():
            load_w(k + 1)

    @pl.loop(0, chunks)
    def _(i):
        begin(i)
        slot = i % 2

        @pl.loop(0, tiles // 2)
        def _(t):
            r = rows_at(t, 2 * TILE)

            @pl.when(i == 0)
            def _():
                copy_x(t).wait()

                @pl.when(t + 1 < tiles // 2)
                def _():
                    copy_x(t + 1).start()

                a[r] = normed(x[r])

            @pl.when((i == 1) & (t == 0))
            def _():
                for k in range(tiles):
                    copy_dy(k).start()

            both = nn(a[r], wgu[slot])
            pairs = [(both[:, lanes_of(2 * k)], both[:, lanes_of(2 * k + 1)]) for k in range(HALVES)]
            hidden = [(gate * jax.nn.sigmoid(gate) * up).astype(BF16) for gate, up in pairs]
            acc[r] = jnp.where(i == 0, 0.0, acc[r]) + nn(jnp.concatenate(hidden, -1), wd[slot])

            @pl.when(i == chunks - 1)
            def _():
                h1[r] = x[r] + acc[r].astype(BF16)
                a[r] = normed(h1[r])

    pl.semaphore_wait(barrier, 2)

    def backward(u, last):
        h, _, i = where(u)
        k = chunks + u // HALVES
        slot = k % 2
        first = u % units == 0
        hidden_units = pl.ds(pl.multiple_of(h * width, width), width)
        pairs = pl.ds(pl.multiple_of(h * 2 * width, width), 2 * width)

        @pl.when(h == 0)
        def _():
            begin(k)

        @pl.loop(0, tiles)
        def _(t):
            r = rows_at(t)

            @pl.when(first)
            def _():
                if last:
                    copy_dy(t).wait()
                else:
                    dy[r] = dy[r] + normed_back(h1[r], acc[r].astype(BF16).astype(F32))
                    a[r] = normed(x[r])

            at, dyt = a[r], dy[r]
            both = nn(at, wgu[slot, :, pairs])
            gate, up = both[:, lanes_of(0)], both[:, lanes_of(1)]
            by_hidden = nt(dyt, wd[slot, hidden_units, :]).astype(BF16).astype(F32)
            sigmoid = jax.nn.sigmoid(gate)
            silu = gate * sigmoid
            hidden = (silu * up).astype(BF16)
            by_up = (by_hidden * silu).astype(BF16)
            by_gate = (by_hidden * up * (sigmoid + silu * (1 - sigmoid))).astype(BF16)
            by_both = jnp.concatenate([by_gate, by_up], -1)
            new = t == 0
            accd[i % 2, :, hidden_units] = jnp.where(new, 0.0, accd[i % 2, :, hidden_units]) + tn(dyt, hidden)
            accgu[h] = jnp.where(new, 0.0, accgu[h]) + tn(at, by_both)
            if last:
                acc[r] = jnp.where(first, 0.0, acc[r]) + nt(by_both, wgu[slot, :, pairs])

            @pl.when(t == 0)
            def _():
                @pl.when(u >= 3)
                def _():
                    finish(u - 3)

                @pl.when(u >= 1)
                def _():
                    sum_2(u - 1)
                    load_mvw(u - 1)

            @pl.when((t == tiles - 2) & (u >= 2))
            def _():
                gather_2(u - 2)

        sum_1(u)

        @pl.when(u >= 1)
        def _():
            sum_3(u - 1)

    @pl.loop(0, units)
    def _(u):
        backward(u, True)

    @pl.loop(units, 2 * units)
    def _(u):
        backward(u, False)

    end = 2 * units - 1
    finish(end - 2)
    sum_2(end)
    load_mvw(end)
    gather_2(end - 1)
    sum_3(end)
    finish(end - 1)
    gather_2(end)
    finish(end)


def pieces_of(shape, dtype):
    layers, height, width = shape
    cut = max(1, height * width * jnp.dtype(dtype).itemsize // 1300000)
    while height % (cut * 8):
        cut -= 1
    return [(l, slice(k * height // cut, (k + 1) * height // cut)) for l in range(layers) for k in range(cut)]


def copies(*refs):
    count = (len(refs) - 2) // 3
    source, target, held = (refs[k * count : (k + 1) * count] for k in range(3))
    in_sem, out_sem = refs[-2:]
    places = [(k, *at) for k, ref in enumerate(source) for at in pieces_of(ref.shape, ref.dtype)]
    way_in = [pltpu.make_async_copy(source[k].at[l, s], held[k].at[l, s], in_sem.at[p]) for p, (k, l, s) in enumerate(places)]
    way_out = [pltpu.make_async_copy(held[k].at[l, s], target[k].at[l, s], out_sem.at[p]) for p, (k, l, s) in enumerate(places)]
    for copy in way_in:
        copy.start()
    for p, copy in enumerate(way_out):
        way_in[p].wait()
        copy.start()
    for copy in way_out:
        copy.wait()


def solution(mesh):
    n = mesh.shape["dp"]
    most = 67043328

    def step(x, dy, *arrays):
        weights, moments = arrays[:3], arrays[3:]
        tokens, d_model = x.shape[1:]
        chunk, rows, half = n * LANES, d_model // n, LANES // 2
        width = chunk // HALVES
        shapes = [jax.ShapeDtypeStruct(w.shape, BF16) for w in weights] + [jax.ShapeDtypeStruct(m.shape, F32) for m in moments]
        vmem, dma = pltpu.VMEM, pltpu.SemaphoreType.DMA
        anywhere = pl.BlockSpec(memory_space=pl.ANY)
        new = pl.pallas_call(
            functools.partial(kernel, n),
            out_shape=shapes,
            in_specs=[anywhere] * 11,
            out_specs=[anywhere] * 9,
            scratch_shapes=[
                vmem((tokens, d_model), BF16),
                vmem((tokens, d_model), BF16),
                vmem((tokens, d_model), BF16),
                vmem((tokens, d_model), BF16),
                vmem((tokens, d_model), F32),
                vmem((HALVES, d_model, 2 * width), F32),
                vmem((2, d_model, chunk), F32),
                vmem((2, d_model, 2 * chunk), BF16),
                vmem((2, chunk, d_model), BF16),
                vmem((2, rows, width), BF16),
                vmem((2, half, d_model), BF16),
                vmem((HALVES, 2, rows, width), BF16),
                vmem((2, half, d_model), BF16),
                vmem((2, 2, rows, width), BF16),
                vmem((2, LANES, d_model), BF16),
                vmem((HALVES, 2, 2, rows, width), BF16),
                vmem((2, LANES, d_model), BF16),
                vmem((HALVES, 2, rows, width), BF16),
                vmem((LANES, d_model), BF16),
                vmem((HALVES, 2, 2, rows, width), F32),
                vmem((2, LANES, d_model), F32),
                dma((2, tokens // TILE)),
                dma((2, 2)),
                dma((2, 3)),
                dma((2, 3)),
                dma((2, 2)),
                dma((HALVES + 1, 2)),
                dma((2, 2)),
                dma((HALVES + 1, 2)),
                dma((HALVES + 1, 2)),
                dma((HALVES + 1, 2)),
                dma((HALVES + 1, 2)),
                dma((HALVES + 1, 2)),
            ],
            compiler_params=pltpu.CompilerParams(
                collective_id=0, has_side_effects=True, vmem_limit_bytes=most,
            ),
            name="train_step",
        )(x, dy, *arrays)
        places = sum(len(pieces_of(s.shape, s.dtype)) for s in shapes)
        return pl.pallas_call(
            copies,
            out_shape=shapes,
            in_specs=[anywhere] * 9,
            out_specs=[anywhere] * 9,
            scratch_shapes=[vmem(s.shape, s.dtype) for s in shapes] + [dma((places,)), dma((places,))],
            compiler_params=pltpu.CompilerParams(vmem_limit_bytes=most),
            name="results",
        )(*new)

    tokens, whole = P(("rep", "dp"), None, None), P(None, None, None)
    shares = [P(None, "dp", None)] * 6
    return jax.shard_map(
        step,
        mesh=mesh,
        in_specs=(tokens, tokens, whole, whole, whole, *shares),
        out_specs=tuple([P("rep", None, None)] * 3 + [P("rep", "dp", None)] * 6),
        check_vma=False,
    )
```
